32 devices in a mesh: dp: 4 (over x, y), sp: 8 (over z, core).
Axes of the slice: x: 2, y: 2, z: 4, core: 2. Of those that a mesh axis runs over, the one named last changes fastest.
Arguments:
- x: bfloat16 [16384, 4096], P(('dp', 'sp')), parts along dimension 0
- gain: bfloat16 [4096], replicated
- wq: bfloat16 [4096, 4096], replicated
- wk: bfloat16 [4096, 4096], replicated
- wv: bfloat16 [4096, 4096], replicated
- wo: bfloat16 [4096, 4096], replicated
Outputs:
- output: bfloat16 [16384, 4096], P(('dp', 'sp')), parts along dimension 0
There are 4 independent parts. The reference program is written for one: setup_inputs(seed, part) draws one part's arguments, and reference() takes and returns one part's arrays. A program takes and returns all parts, laid end to end along the dimension named above; an argument that names none is the same for every part.
All inputs are finite; a program needn't handle non-finite values.
Results may differ from the reference program's by a relative error of at most 0.012.
Values are sent between devices in bfloat16 or wider.
A program may use at most 2 GiB of HBM per device.

```python
import jax
import jax.numpy as jnp
from jax import lax

ROWS = 4096
D = 4096
HEADS = 16
KV_HEADS = 16
HEAD = 256
THETA = 10000


def setup_inputs(seed: int = 0, part: int = 0) -> dict:
    kx, kn, kq, kk, kv, ko = jax.random.split(jax.random.key(seed), 6)

    def weights(key, rows, columns):
        return jax.random.normal(key, (rows, columns), jnp.float32) * rows**-0.5

    drawn = {
        "x": jax.random.normal(jax.random.fold_in(kx, part), (ROWS, D), jnp.float32),
        "gain": 1 + 0.1 * jax.random.normal(kn, (D,), jnp.float32),
        "wq": 2 * weights(kq, D, HEADS * HEAD),
        "wk": 2 * weights(kk, D, KV_HEADS * HEAD),
        "wv": 4 * weights(kv, D, KV_HEADS * HEAD),
        "wo": weights(ko, HEADS * HEAD, D),
    }
    return {k: v.astype(jnp.bfloat16) for k, v in drawn.items()}


def normed(x, gain):
    wide = x.astype(jnp.float32)
    scale = lax.rsqrt(jnp.mean(wide * wide, -1, keepdims=True) + 1e-6)
    return (wide * scale * gain.astype(jnp.float32)).astype(jnp.bfloat16)


def turned(t, place, theta):
    half = t.shape[-1] // 2
    angle = place.astype(jnp.float32)[:, None] * theta ** (-jnp.arange(half, dtype=jnp.float32) / half)
    cos, sin = jnp.cos(angle)[:, None], jnp.sin(angle)[:, None]
    a, b = t[..., :half].astype(jnp.float32), t[..., half:].astype(jnp.float32)
    return jnp.concatenate([a * cos - b * sin, b * cos + a * sin], -1).astype(jnp.bfloat16)


def matmul(a, w):
    return jnp.dot(a, w, preferred_element_type=jnp.float32).astype(jnp.bfloat16)


def einsum(form, a, b):
    return jnp.einsum(form, a.astype(jnp.float32), b.astype(jnp.float32))


def attention(q, k, v):
    scores = einsum("tgsd,ugd->gstu", q, k) * q.shape[-1] ** -0.5
    token = jnp.arange(q.shape[0])
    scores = jnp.where(token[:, None] >= token, scores, -jnp.inf)
    weights = jax.nn.softmax(scores, -1).astype(jnp.bfloat16)
    return einsum("gstu,ugd->tgsd", weights, v).astype(jnp.bfloat16)


def reference(x, gain, wq, wk, wv, wo):
    a, place = normed(x, gain), jnp.arange(ROWS)
    q = turned(matmul(a, wq).reshape(ROWS, HEADS, HEAD), place, THETA).reshape(ROWS, KV_HEADS, -1, HEAD)
    k = turned(matmul(a, wk).reshape(ROWS, KV_HEADS, HEAD), place, THETA)
    v = matmul(a, wv).reshape(ROWS, KV_HEADS, HEAD)
    seen = attention(q, k, v).reshape(ROWS, HEADS * HEAD)
    return (x.astype(jnp.float32) + jnp.dot(seen, wo, preferred_element_type=jnp.float32)).astype(jnp.bfloat16)
```

```python
import functools

import jax
import jax.numpy as jnp
from jax import lax
from jax.experimental import pallas as pl
from jax.experimental.pallas import tpu as pltpu
from jax.sharding import PartitionSpec as P

HEAD = 256
HALF = HEAD // 2
THETA = 10000
NEG = -1e30
HIDDEN = 2 * NEG
LOG2E = 1.4426950408889634
SCALE = HEAD**-0.5
E2 = SCALE * LOG2E
VMEM = 67_000_000 // 1024 * 1024
BK = 512
STRIP = 512

def normed(x, gain):
    wide = x.astype(jnp.float32)
    scale = lax.rsqrt(jnp.mean(wide * wide, -1, keepdims=True) + 1e-6)
    return (wide * scale * gain.astype(jnp.float32)).astype(jnp.bfloat16)


def _dot(a, b, ca, cb):
    return lax.dot_general(a, b, (((ca,), (cb,)), ((), ())), preferred_element_type=jnp.float32)


LOCAL = 8
PAIRS = LOCAL // 2
WIDE = 2 * HEAD


def _block(k, v, strips, top_s, mix_s, masks=None):
    values = jnp.concatenate([v.T, jnp.ones((8, k.shape[0]), k.dtype)], axis=0)
    scores = [_dot(k, q, 1, 1) for _, q in strips]
    weights, keeps = [], []
    for n, ((i, _), s) in enumerate(zip(strips, scores)):
        if masks is not None:
            s = jnp.where(masks[n], s, HIDDEN)
        old = top_s[i]
        top = jnp.maximum(old, s.max(axis=0, keepdims=True))
        top_s[i] = top
        weights.append(jnp.exp2((s - top) * E2).astype(k.dtype))
        keeps.append(jnp.exp2((old - top) * E2))
    for (i, _), p, keep in zip(strips, weights, keeps):
        mix_s[i] = mix_s[i] * keep + _dot(values, p, 1, 0)


def _clear(i, top_s, mix_s):
    top_s[i] = jnp.full((1, STRIP), NEG, jnp.float32)
    mix_s[i] = jnp.zeros((HEAD + 8, STRIP), jnp.float32)


def _result(i, top_s, mix_s):
    total = mix_s[i, HEAD : HEAD + 1, :]
    return (mix_s[i, :HEAD, :] * (1 / total)).T.astype(jnp.bfloat16), top_s[i] * SCALE + jnp.log(total)


def _part(i):
    return slice(i * STRIP, (i + 1) * STRIP)


def _main(
    a_ref, cos_ref, sin_ref, wq_ref, wk_ref, wv_ref, kept_ref, got_ref,
    a_s, w_s, qkv, recv, lse_s, lse_r, top_s, mix_s, sem_a, sem_w, send_s, recv_s, lsend_s, lrecv_s, out_s,
):
    s = lax.axis_index("sp")
    z, c = s // 2, s % 2
    other = s + 1 - 2 * c
    rows = a_ref.shape[0]
    remote = functools.partial(pltpu.make_async_remote_copy, device_id_type=pl.DeviceIdType.MESH)

    def queries_one_down(h):
        return remote(qkv.at[h, 0], recv.at[h, 0], send_s.at[h, 2], recv_s.at[h, 0], device_id={"sp": s - 2})

    def queries_two_down(h):
        return remote(qkv.at[h, 0], recv.at[h, 1], send_s.at[h, 3], recv_s.at[h, 1], device_id={"sp": s - 4})

    def keys_up(h):
        return remote(qkv.at[h, pl.ds(1, 2)], recv.at[h, pl.ds(2, 2)], send_s.at[h, 2], recv_s.at[h, 2], device_id={"sp": s + 2})

    def part_one_up(h):
        return (
            remote(recv.at[h, 0], recv.at[h, 2], send_s.at[h, 0], recv_s.at[h, 2], device_id={"sp": s + 2}),
            remote(lse_s.at[h, 0], lse_r.at[h, 0], lsend_s.at[h, 0], lrecv_s.at[h, 0], device_id={"sp": s + 2}),
        )

    def part_two_up(h):
        return (
            remote(recv.at[h, 1], recv.at[h, 3], send_s.at[h, 1], recv_s.at[h, 3], device_id={"sp": s + 4}),
            remote(lse_s.at[h, 1], lse_r.at[h, 1], lsend_s.at[h, 1], lrecv_s.at[h, 1], device_id={"sp": s + 4}),
        )

    def result_keep(h):
        return pltpu.make_async_copy(qkv.at[h, 0, pl.ds(0, rows)], kept_ref.at[h], out_s.at[h, 0])

    def result_give(h):
        return remote(qkv.at[h, 0, pl.ds(rows, rows)], got_ref.at[h], out_s.at[h, 1], out_s.at[h, 2], device_id={"sp": other})

    barrier = pltpu.get_barrier_semaphore()
    for n in range(1, 8):
        pl.semaphore_signal(barrier, inc=1, device_id={"sp": lax.rem(s + n, 8)}, device_id_type=pl.DeviceIdType.MESH)
    pl.semaphore_wait(barrier, 7)

    a_in = pltpu.make_async_copy(a_ref, a_s.at[pl.ds(0, rows)], sem_a.at[0])
    a_over = remote(a_ref, a_s.at[pl.ds(rows, rows)], sem_a.at[1], sem_a.at[2], device_id={"sp": other})

    def weights(kind, p, slot):
        at = pl.multiple_of((c * PAIRS + p) * WIDE, WIDE)
        return pltpu.make_async_copy((wq_ref, wk_ref, wv_ref)[kind].at[:, pl.ds(at, WIDE)], w_s.at[slot], sem_w.at[slot])

    a_in.start()
    weights(0, 0, 0).start()
    a_over.start()
    weights(1, 0, 1).start()

    def project(p):
        for kind in range(3):
            slot = lax.rem(3 * p + kind, 2)
            weights(kind, p, slot).wait()

            def half(m, _):
                @pl.when((p == 0) & (kind == 0) & (m == 0))
                def _():
                    a_in.wait()

                @pl.when((p == 0) & (kind == 0) & (m == 1))
                def _():
                    a_over.wait_recv()

                here = pl.ds(pl.multiple_of(m * rows, rows), rows)
                t = _dot(a_s[here, :], w_s[slot], 1, 0)
                if kind < 2:
                    cos, sin = cos_ref[here, :], sin_ref[here, :]
                for i in range(2):
                    u = t[:, i * HEAD : (i + 1) * HEAD].astype(jnp.bfloat16)
                    if kind < 2:
                        u = u.astype(jnp.float32)
                        a, b = u[:, :HALF], u[:, HALF:]
                        u = jnp.concatenate([a * cos - b * sin, b * cos + a * sin], axis=1).astype(jnp.bfloat16)
                    qkv[2 * p + i, kind, here, :] = u

            lax.fori_loop(0, 2, half, None)
            ahead = (kind + 2) % 3
            if ahead == 2:
                weights(2, p, slot).start()
            else:

                @pl.when(p < PAIRS - 1)
                def _():
                    weights(ahead, p + 1, slot).start()

            if kind == 0:
                for i in range(2):

                    @pl.when(z >= 2)
                    def _():
                        queries_one_down(2 * p + i).start()

                    @pl.when(z == 3)
                    def _():
                        queries_two_down(2 * p + i).start()

            if kind == 2:

                @pl.when(z == 0)
                def _():
                    for i in range(2):
                        keys_up(2 * p + i).start()

    def over(ref, h, at, strips):
        def body(j, _):
            here = pl.ds(pl.multiple_of(j * BK, BK), BK)
            _block(ref[h, at, here, :], ref[h, at + 1, here, :], strips(), top_s, mix_s)

        lax.fori_loop(0, 2 * rows // BK, body, None)

    def serve(h):
        one = lambda: [(i, recv[h, 0, _part(i), :]) for i in range(2)]
        both = lambda: one() + [(2 + i, recv[h, 1, _part(i), :]) for i in range(2)]
        queries_one_down(h).wait_recv()
        for i in range(2):
            _clear(i, top_s, mix_s)

        @pl.when(z == 1)
        def _():
            queries_two_down(h).wait_recv()
            keys_up(h).wait_recv()
            for i in range(2, 4):
                _clear(i, top_s, mix_s)
            over(recv, h, 2, both)
            over(qkv, h, 1, both)

        @pl.when(z == 2)
        def _():
            over(qkv, h, 1, one)

        for i in range(2):
            recv[h, 0, _part(i), :], lse_s[h, 0, :, _part(i)] = _result(i, top_s, mix_s)
        for copy in part_one_up(h):
            copy.start()

        @pl.when(z == 1)
        def _():
            for i in range(2):
                recv[h, 1, _part(i), :], lse_s[h, 1, :, _part(i)] = _result(2 + i, top_s, mix_s)
            for copy in part_two_up(h):
                copy.start()

    def attend_own(h):
        one = lambda i: [(i, qkv[h, 0, _part(i), :])]

        @pl.when(z < 2)
        def _():
            for i in range(2):
                _clear(i, top_s, mix_s)

        @pl.when(z == 1)
        def _():
            over(recv, h, 2, lambda: one(0) + one(1))

        @pl.when(z >= 2)
        def _():
            for copy in part_one_up(h):
                copy.wait_recv()
            queries_one_down(h).wait_send()

            @pl.when(z == 2)
            def _():
                for i in range(2):
                    la = lse_r[h, 0, :, _part(i)]
                    top_s[i] = la * (1 / SCALE)
                    mix_s[i, :HEAD, :] = recv[h, 2, _part(i), :].astype(jnp.float32).T
                    mix_s[i, HEAD:, :] = jnp.ones((8, STRIP), jnp.float32)

            @pl.when(z == 3)
            def _():
                for copy in part_two_up(h):
                    copy.wait_recv()
                queries_two_down(h).wait_send()
                for i in range(2):
                    la, lb = lse_r[h, 0, :, _part(i)], lse_r[h, 1, :, _part(i)]
                    top = jnp.maximum(la, lb)
                    wa, wb = jnp.exp(la - top), jnp.exp(lb - top)
                    top_s[i] = top * (1 / SCALE)
                    mix_s[i, :HEAD, :] = recv[h, 2, _part(i), :].astype(jnp.float32).T * wa + recv[h, 3, _part(i), :].astype(jnp.float32).T * wb
                    mix_s[i, HEAD:, :] = jnp.broadcast_to(wa + wb, (8, STRIP))

        early = pl.ds(pl.multiple_of(c * STRIP, STRIP), STRIP)
        late = 1 - c
        at = pl.ds(pl.multiple_of(late * STRIP, STRIP), STRIP)
        _block(qkv[h, 1, early, :], qkv[h, 2, early, :], [(late, qkv[h, 0, at, :])], top_s, mix_s)
        seen = lax.broadcasted_iota(jnp.int32, (STRIP, STRIP), 1) >= lax.broadcasted_iota(jnp.int32, (STRIP, STRIP), 0)
        for i in range(2):
            _block(qkv[h, 1, _part(i), :], qkv[h, 2, _part(i), :], one(i), top_s, mix_s, [seen])
        for i in range(2):
            qkv[h, 0, _part(i), :], _ = _result(i, top_s, mix_s)
        result_keep(h).start()
        result_give(h).start()

    def turn(t, _):
        @pl.when(t < PAIRS)
        def _():
            project(t)

        @pl.when((t >= 1) & (t <= LOCAL) & ((z == 1) | (z == 2)))
        def _():
            serve(t - 1)

        h = t - jnp.where(z < 2, 1, 4)

        @pl.when((h >= 0) & (h < LOCAL))
        def _():
            attend_own(h)

    lax.fori_loop(0, LOCAL + 4, turn, None)
    a_over.wait_send()

    def finish(h, _):
        result_keep(h).wait()
        result_give(h).wait()

        @pl.when(z == 0)
        def _():
            keys_up(h).wait_send()

        @pl.when((z == 1) | (z == 2))
        def _():
            for copy in part_one_up(h):
                copy.wait_send()

        @pl.when(z == 1)
        def _():
            for copy in part_two_up(h):
                copy.wait_send()

    lax.fori_loop(0, LOCAL, finish, None)


def project_and_attend(a, cos, sin, wq, wk, wv):
    rows, d = a.shape
    hbm, vmem = pl.BlockSpec(memory_space=pl.ANY), pl.BlockSpec(memory_space=pltpu.VMEM)
    dma = pltpu.SemaphoreType.DMA
    t = 2 * rows
    return pl.pallas_call(
        _main,
        in_specs=[hbm, vmem, vmem, hbm, hbm, hbm],
        out_specs=[hbm, hbm],
        out_shape=[jax.ShapeDtypeStruct((LOCAL, rows, HEAD), jnp.bfloat16)] * 2,
        scratch_shapes=[
            pltpu.VMEM((t, d), jnp.bfloat16),
            pltpu.VMEM((2, d, WIDE), jnp.bfloat16),
            pltpu.VMEM((LOCAL, 3, t, HEAD), jnp.bfloat16),
            pltpu.VMEM((LOCAL, 4, t, HEAD), jnp.bfloat16),
            pltpu.VMEM((LOCAL, 2, 1, t), jnp.float32),
            pltpu.VMEM((LOCAL, 2, 1, t), jnp.float32),
            pltpu.VMEM((4, 1, STRIP), jnp.float32),
            pltpu.VMEM((4, HEAD + 8, STRIP), jnp.float32),
            dma((3,)),
            dma((2,)),
            dma((LOCAL, 4)),
            dma((LOCAL, 4)),
            dma((LOCAL, 2)),
            dma((LOCAL, 2)),
            dma((LOCAL, 3)),
        ],
        compiler_params=pltpu.CompilerParams(collective_id=0, has_side_effects=True, vmem_limit_bytes=VMEM),
        cost_estimate=pl.CostEstimate(flops=2 * t * d * 3 * HEAD * LOCAL, transcendentals=0, bytes_accessed=2 * (t * d + 3 * d * HEAD * LOCAL)),
        name="project_and_attend",
    )(a, cos, sin, wq, wk, wv)


def _out(meta_ref, x_ref, kept_ref, got_ref, wa_ref, wb_ref, y_ref, o_s):
    @pl.when(pl.program_id(0) == 0)
    def _():
        for h in range(LOCAL):
            o_s[0, :, h * HEAD : (h + 1) * HEAD] = kept_ref[h]
            o_s[1, :, h * HEAD : (h + 1) * HEAD] = got_ref[h]

    acc = _dot(o_s[0], wa_ref[...], 1, 0) + _dot(o_s[1], wb_ref[...], 1, 0)
    y_ref[...] = (x_ref[...].astype(jnp.float32) + acc).astype(y_ref.dtype)


def out(meta, x, kept, got, wo, wide=512):
    rows, d = x.shape
    whole = pl.BlockSpec(kept.shape, lambda n, m: (0, 0, 0))
    block = pl.BlockSpec((rows, wide), lambda n, m: (0, n))
    w = lambda side: pl.BlockSpec((d // 2, wide), lambda n, m: (m[1] if side == 0 else 1 - m[1], n))
    return pl.pallas_call(
        _out,
        grid_spec=pltpu.PrefetchScalarGridSpec(
            num_scalar_prefetch=1,
            grid=(d // wide,),
            in_specs=[block, whole, whole, w(0), w(1)],
            out_specs=block,
            scratch_shapes=[pltpu.VMEM((2, rows, d // 2), jnp.bfloat16)],
        ),
        out_shape=jax.ShapeDtypeStruct((rows, d), x.dtype),
        compiler_params=pltpu.CompilerParams(dimension_semantics=("arbitrary",), vmem_limit_bytes=56 * 2**20),
        cost_estimate=pl.CostEstimate(flops=2 * rows * d * d, transcendentals=0, bytes_accessed=2 * d * d + 4 * rows * d),
        name="out",
    )(meta, x, kept, got, wo, wo)


def solution(mesh):
    def step(x, gain, wq, wk, wv, wo):
        rows = x.shape[0]
        s = lax.axis_index("sp")
        meta = jnp.stack([s // 2, s % 2]).astype(jnp.int32)
        a = normed(x, gain)
        place = jnp.concatenate([s * rows + jnp.arange(rows), (s + 1 - 2 * (s % 2)) * rows + jnp.arange(rows)])
        angle = place.astype(jnp.float32)[:, None] * THETA ** (-jnp.arange(HALF, dtype=jnp.float32) / HALF)
        kept, got = project_and_attend(a, jnp.cos(angle), jnp.sin(angle), wq, wk, wv)
        return out(meta, x, kept, got, wo)

    tokens, whole = P(("dp", "sp"), None), P(None, None)
    return jax.shard_map(
        step,
        mesh=mesh,
        in_specs=(tokens, P(None), whole, whole, whole, whole),
        out_specs=tokens,
        check_vma=False,
    )
```

```python
import functools

import jax
import jax.numpy as jnp
import numpy as np
from jax import lax
from jax.experimental import pallas as pl
from jax.experimental.pallas import tpu as pltpu
from jax.sharding import PartitionSpec as P

HEAD = 256
HALF = HEAD // 2
THETA = 10000
NEG = -1e30
HIDDEN = 2 * NEG
LOG2E = 1.4426950408889634
SCALE = HEAD**-0.5
E2 = SCALE * LOG2E
VMEM = 67_000_000 // 1024 * 1024
BK = 512
STRIP = 512

def _dot(a, b, ca, cb):
    return lax.dot_general(a, b, (((ca,), (cb,)), ((), ())), preferred_element_type=jnp.float32)


LOCAL = 8
PAIRS = LOCAL // 2
WIDE = 2 * HEAD


def _block(k, v, strips, top_s, mix_s, masks=None):
    values = jnp.concatenate([v.T, jnp.ones((8, k.shape[0]), k.dtype)], axis=0)
    scores = [_dot(k, q, 1, 1) for _, q in strips]
    weights, keeps = [], []
    for n, ((i, _), s) in enumerate(zip(strips, scores)):
        if masks is not None:
            s = jnp.where(masks[n], s, HIDDEN)
        old = top_s[i]
        top = jnp.maximum(old, s.max(axis=0, keepdims=True))
        top_s[i] = top
        weights.append(jnp.exp2((s - top) * E2).astype(k.dtype))
        keeps.append(jnp.exp2((old - top) * E2))
    for (i, _), p, keep in zip(strips, weights, keeps):
        mix_s[i] = mix_s[i] * keep + _dot(values, p, 1, 0)


def _clear(i, top_s, mix_s):
    top_s[i] = jnp.full((1, STRIP), NEG, jnp.float32)
    mix_s[i] = jnp.zeros((HEAD + 8, STRIP), jnp.float32)


def _result(i, top_s, mix_s):
    total = mix_s[i, HEAD : HEAD + 1, :]
    return (mix_s[i, :HEAD, :] * (1 / total)).T.astype(jnp.bfloat16), top_s[i] * SCALE + jnp.log(total)


def _part(i):
    return slice(i * STRIP, (i + 1) * STRIP)


def _main(
    x_ref, gain_ref, near_ref, far_ref, wq_ref, wk_ref, wv_ref, wo_ref, y_ref,
    a_s, w_s, qkv, recv, lse_s, lse_r, top_s, mix_s, cos_ref, sin_ref, o_s, y_s,
    sem_a, sem_w, send_s, recv_s, lsend_s, lrecv_s, out_s, sem_y,
):
    s = lax.axis_index("sp")
    z, c = s // 2, s % 2
    other = s + 1 - 2 * c
    rows = x_ref.shape[0]
    remote = functools.partial(pltpu.make_async_remote_copy, device_id_type=pl.DeviceIdType.MESH)

    def queries_one_down(h):
        return remote(qkv.at[h, 0], recv.at[h, 0], send_s.at[h, 2], recv_s.at[h, 0], device_id={"sp": s - 2})

    def queries_on(h):
        return remote(recv.at[h, 0], recv.at[h, 1], send_s.at[h, 3], recv_s.at[h, 1], device_id={"sp": s - 2})

    def keys_up(h):
        return remote(qkv.at[h, 1], recv.at[h, 2], send_s.at[h, 2], recv_s.at[h, 2], device_id={"sp": s + 2})

    def values_up(h):
        return remote(qkv.at[h, 2], recv.at[h, 3], send_s.at[h, 3], recv_s.at[h, 3], device_id={"sp": s + 2})

    def part_one_up(h):
        return (
            remote(recv.at[h, lax.rem(z + 1, 2)], recv.at[h, 2], send_s.at[h, 0], recv_s.at[h, 2], device_id={"sp": s + 2}),
            remote(lse_s.at[h, 0], lse_r.at[h, 0], lsend_s.at[h, 0], lrecv_s.at[h, 0], device_id={"sp": s + 2}),
        )

    def part_two_up(h):
        return (
            remote(recv.at[h, 1], recv.at[h, 3], send_s.at[h, 1], recv_s.at[h, 3], device_id={"sp": s + 4}),
            remote(lse_s.at[h, 1], lse_r.at[h, 1], lsend_s.at[h, 1], lrecv_s.at[h, 1], device_id={"sp": s + 4}),
        )

    def give(h):
        return remote(qkv.at[h, 0, pl.ds(rows, rows)], o_s.at[h, :, pl.ds(HEAD, HEAD)], out_s.at[h, 0], out_s.at[h, 1], device_id={"sp": other})

    a_in = pltpu.make_async_copy(x_ref, a_s.at[pl.ds(0, rows)], sem_a.at[0])
    a_over = remote(x_ref, a_s.at[pl.ds(rows, rows)], sem_a.at[1], sem_a.at[2], device_id={"sp": other})

    lower = z < 2
    kind_0 = jnp.where(lower, 1 - c, c)
    kind_1 = jnp.where(lower, 2 - c, 1 + c)
    kind_2 = 3 - kind_0 - kind_1

    def kind_at(j):
        return jnp.where(j == 0, kind_0, jnp.where(j == 1, kind_1, kind_2))

    def start_weights(tile):
        p, j = tile // 3, lax.rem(tile, 3)
        at = pl.ds(pl.multiple_of((c * PAIRS + p) * WIDE, WIDE), WIDE)
        slot, kind = lax.rem(tile, 2), kind_at(j)
        for n, w in enumerate((wq_ref, wk_ref, wv_ref)):

            @pl.when(kind == n)
            def _():
                pltpu.make_async_copy(w.at[:, at], w_s.at[slot], sem_w.at[slot]).start()

    def wait_weights(slot):
        pltpu.make_async_copy(wq_ref.at[:, pl.ds(0, WIDE)], w_s.at[slot], sem_w.at[slot]).wait()

    a_in.start()
    start_weights(jnp.int32(0))
    start_weights(jnp.int32(1))

    barrier = pltpu.get_barrier_semaphore()
    for n in range(1, 8):
        pl.semaphore_signal(barrier, inc=1, device_id={"sp": lax.rem(s + n, 8)}, device_id_type=pl.DeviceIdType.MESH)
    pl.semaphore_wait(barrier, 7)
    a_over.start()

    y_s[...] = jnp.zeros_like(y_s)
    for i, place in enumerate((s, other)):
        cos, sin = far_ref[0, pl.ds(place, 1), :], far_ref[1, pl.ds(place, 1), :]
        here = pl.ds(i * rows, rows)
        cos_ref[here, :] = near_ref[0] * cos - near_ref[1] * sin
        sin_ref[here, :] = near_ref[1] * cos + near_ref[0] * sin

    gain = gain_ref[...].astype(jnp.float32)[None, :]

    def norm(first):
        def body(i, _):
            here = pl.ds(pl.multiple_of(first + i * 32, 32), 32)
            wide = a_s[here, :].astype(jnp.float32)
            scale = lax.rsqrt(jnp.mean(wide * wide, -1, keepdims=True) + 1e-6)
            a_s[here, :] = (wide * scale * gain).astype(jnp.bfloat16)

        lax.fori_loop(0, rows // 32, body, None)

    a_in.wait()
    norm(0)

    def project(p):
        def one_kind(j, _):
            tile = 3 * p + j
            kind = kind_at(j)
            slot = lax.rem(tile, 2)
            wait_weights(slot)

            def half(m, _):
                @pl.when((tile == 0) & (m == 1))
                def _():
                    a_over.wait_recv()
                    norm(rows)

                here = pl.ds(pl.multiple_of(m * rows, rows), rows)
                t = _dot(a_s[here, :], w_s[slot], 1, 0)
                cos, sin = cos_ref[here, :], sin_ref[here, :]
                for i in range(2):
                    u = t[:, i * HEAD : (i + 1) * HEAD].astype(jnp.bfloat16)

                    @pl.when(kind == 2)
                    def _():
                        qkv[2 * p + i, 2, here, :] = u

                    @pl.when(kind < 2)
                    def _():
                        v = u.astype(jnp.float32)
                        a, b = v[:, :HALF], v[:, HALF:]
                        qkv[2 * p + i, kind, here, :] = jnp.concatenate([a * cos - b * sin, b * cos + a * sin], axis=1).astype(jnp.bfloat16)

            lax.fori_loop(0, 2, half, None)

            @pl.when(tile + 2 < 3 * PAIRS)
            def _():
                start_weights(tile + 2)

            @pl.when((kind == 0) & ((z == 3) | ((z == 2) & (p == 0))))
            def _():
                queries_one_down(2 * p).start()

            @pl.when((z == 3) & (j == 2))
            def _():
                queries_one_down(2 * p + 1).start()

            @pl.when((z == 0) & (kind == 1))
            def _():
                keys_up(2 * p).start()

            @pl.when((z == 0) & (kind == 2))
            def _():
                values_up(2 * p).start()
                keys_up(2 * p + 1).start()
                values_up(2 * p + 1).start()

        lax.fori_loop(0, 3, one_kind, None)

    def over(ref, h, at, strips):
        def body(j, _):
            here = pl.ds(pl.multiple_of(j * BK, BK), BK)
            _block(ref[h, at, here, :], ref[h, at + 1, here, :], strips(), top_s, mix_s)

        lax.fori_loop(0, 2 * rows // BK, body, None)

    def serve(h):
        one = lambda: [(i, recv[h, 0, _part(i), :]) for i in range(2)]
        both = lambda: one() + [(2 + i, recv[h, 1, _part(i), :]) for i in range(2)]
        for i in range(2):
            _clear(i, top_s, mix_s)

        @pl.when(z == 1)
        def _():
            queries_one_down(h).wait_recv()
            queries_on(h).wait_recv()
            for i in range(2, 4):
                _clear(i, top_s, mix_s)
            over(qkv, h, 1, both)
            keys_up(h).wait_recv()
            values_up(h).wait_recv()
            over(recv, h, 2, both)

        @pl.when(z == 2)
        def _():
            over(qkv, h, 1, one)

        for i in range(2):
            recv[h, lax.rem(z + 1, 2), _part(i), :], lse_s[h, 0, :, _part(i)] = _result(i, top_s, mix_s)
        for copy in part_one_up(h):
            copy.start()

        @pl.when(z == 1)
        def _():
            for i in range(2):
                recv[h, 1, _part(i), :], lse_s[h, 1, :, _part(i)] = _result(2 + i, top_s, mix_s)
            for copy in part_two_up(h):
                copy.start()

    def attend_own(h, _):
        one = lambda i: [(i, qkv[h, 0, _part(i), :])]

        @pl.when(z < 2)
        def _():
            for i in range(2):
                _clear(i, top_s, mix_s)

        @pl.when(z == 1)
        def _():
            over(recv, h, 2, lambda: one(0) + one(1))

        @pl.when(z >= 2)
        def _():
            for copy in part_one_up(h):
                copy.wait_recv()
            queries_one_down(h).wait_send()

            @pl.when(z == 2)
            def _():
                for i in range(2):
                    la = lse_r[h, 0, :, _part(i)]
                    top_s[i] = la * (1 / SCALE)
                    mix_s[i, :HEAD, :] = recv[h, 2, _part(i), :].astype(jnp.float32).T
                    mix_s[i, HEAD:, :] = jnp.ones((8, STRIP), jnp.float32)

            @pl.when(z == 3)
            def _():
                for copy in part_two_up(h):
                    copy.wait_recv()
                for i in range(2):
                    la, lb = lse_r[h, 0, :, _part(i)], lse_r[h, 1, :, _part(i)]
                    top = jnp.maximum(la, lb)
                    wa, wb = jnp.exp(la - top), jnp.exp(lb - top)
                    top_s[i] = top * (1 / SCALE)
                    mix_s[i, :HEAD, :] = recv[h, 2, _part(i), :].astype(jnp.float32).T * wa + recv[h, 3, _part(i), :].astype(jnp.float32).T * wb
                    mix_s[i, HEAD:, :] = jnp.broadcast_to(wa + wb, (8, STRIP))

        early = pl.ds(pl.multiple_of(c * STRIP, STRIP), STRIP)
        late = 1 - c
        at = pl.ds(pl.multiple_of(late * STRIP, STRIP), STRIP)
        _block(qkv[h, 1, early, :], qkv[h, 2, early, :], [(late, qkv[h, 0, at, :])], top_s, mix_s)
        seen = lax.broadcasted_iota(jnp.int32, (STRIP, STRIP), 1) >= lax.broadcasted_iota(jnp.int32, (STRIP, STRIP), 0)
        for i in range(2):
            _block(qkv[h, 1, _part(i), :], qkv[h, 2, _part(i), :], one(i), top_s, mix_s, [seen])
        o_s[h, :, :HEAD], _ = _result(0, top_s, mix_s)
        qkv[h, 0, _part(1), :], _ = _result(1, top_s, mix_s)
        give(h).start()

    blocks = wo_ref.shape[1] // WIDE
    x_in = pltpu.make_async_copy(x_ref, a_s.at[pl.ds(0, rows)], sem_a.at[0])

    def start_out(h):
        def body(n, _):
            at = pl.ds(pl.multiple_of(n * WIDE, WIDE), WIDE)
            for side, core in enumerate((c, 1 - c)):
                pltpu.make_async_copy(
                    wo_ref.at[pl.ds(pl.multiple_of((core * LOCAL + h) * HEAD, HEAD), HEAD), at],
                    w_s.at[lax.rem(h, 2), pl.ds(pl.multiple_of(n * WIDE + side * HEAD, HEAD), HEAD)],
                    sem_w.at[lax.rem(h, 2)],
                ).start()

        lax.fori_loop(0, blocks, body, None)

    def out_part(h, _, final):
        slot = lax.rem(h, 2)
        give(h).wait_recv()
        wait_weights(slot)

        if final:
            x_in.wait()

        def body(n, _):
            at = pl.ds(pl.multiple_of(n * WIDE, WIDE), WIDE)
            y_s[n] = y_s[n] + _dot(o_s[h], w_s[slot, at, :], 1, 0)

        def last(n, _):
            at = pl.ds(pl.multiple_of(n * WIDE, WIDE), WIDE)
            y = y_s[n] + _dot(o_s[h], w_s[slot, at, :], 1, 0)
            a_s[pl.ds(rows, rows), at] = (a_s[pl.ds(0, rows), at].astype(jnp.float32) + y).astype(jnp.bfloat16)
            pltpu.make_async_copy(a_s.at[pl.ds(rows, rows), at], y_ref.at[:, at], sem_y.at[0]).start()

        lax.fori_loop(0, blocks, last if final else body, None, unroll=2)

        @pl.when(h < LOCAL - 2)
        def _():
            start_out(h + 2)

    def turn(i, _):
        t = i - 1
        p = t + jnp.where((z == 1) & (c == 1), 1, 0)

        @pl.when((p >= 0) & (p < PAIRS))
        def _():
            project(p)

        @pl.when(p == PAIRS - 1)
        def _():
            x_in.start()
            start_out(jnp.int32(0))
            start_out(jnp.int32(1))

        def pass_on(h):
            queries_one_down(h).wait_recv()
            queries_on(h).start()

        @pl.when((z == 2) & (t == 0))
        def _():
            pass_on(0)

        @pl.when((t >= 0) & (t < LOCAL) & ((z == 1) | (z == 2)))
        def _():
            serve(t)

        @pl.when((z == 2) & (t >= 0) & (t < LOCAL - 1))
        def _():
            queries_one_down(t + 1).start()
            pass_on(t + 1)

        def parts(t):
            return jnp.clip(jnp.where(z == 0, 2 * t - 7, jnp.where(z == 1, 2 * t - 9, t - 2)), 0, LOCAL - 1)

        def heads(t):
            return jnp.clip(jnp.where(z == 0, t + 1, jnp.where(z == 1, jnp.where(t < 4, 0, jnp.maximum(t, 3)) - jnp.where(t == 4, 1, 0), t - 1)), 0, LOCAL)

        lax.fori_loop(parts(t - 1), parts(t), functools.partial(out_part, final=False), None)
        lax.fori_loop(heads(t - 1), heads(t), attend_own, None)

    lax.fori_loop(0, LOCAL + 3, turn, None)
    out_part(jnp.int32(LOCAL - 1), None, final=True)
    a_over.wait_send()
    pltpu.make_async_copy(a_s.at[pl.ds(rows, rows)], y_ref, sem_y.at[0]).wait()

    def finish(h, _):
        give(h).wait_send()

        @pl.when(z == 0)
        def _():
            keys_up(h).wait_send()
            values_up(h).wait_send()

        @pl.when((z == 1) | (z == 2))
        def _():
            for copy in part_one_up(h):
                copy.wait_send()

        @pl.when(z == 1)
        def _():
            for copy in part_two_up(h):
                copy.wait_send()

        @pl.when(z == 2)
        def _():
            queries_on(h).wait_send()

    lax.fori_loop(0, LOCAL, finish, None)


def attention_half(x, gain, near, far, wq, wk, wv, wo):
    rows, d = x.shape
    hbm, vmem = pl.BlockSpec(memory_space=pl.ANY), pl.BlockSpec(memory_space=pltpu.VMEM)
    dma = pltpu.SemaphoreType.DMA
    t = 2 * rows
    return pl.pallas_call(
        _main,
        in_specs=[hbm, vmem, vmem, vmem, hbm, hbm, hbm, hbm],
        out_specs=hbm,
        out_shape=jax.ShapeDtypeStruct((rows, d), jnp.bfloat16),
        scratch_shapes=[
            pltpu.VMEM((t, d), jnp.bfloat16),
            pltpu.VMEM((2, d, WIDE), jnp.bfloat16),
            pltpu.VMEM((LOCAL, 3, t, HEAD), jnp.bfloat16),
            pltpu.VMEM((LOCAL, 4, t, HEAD), jnp.bfloat16),
            pltpu.VMEM((LOCAL, 2, 1, t), jnp.float32),
            pltpu.VMEM((LOCAL, 2, 1, t), jnp.float32),
            pltpu.VMEM((4, 1, STRIP), jnp.float32),
            pltpu.VMEM((4, HEAD + 8, STRIP), jnp.float32),
            pltpu.VMEM((t, HALF), jnp.float32),
            pltpu.VMEM((t, HALF), jnp.float32),
            pltpu.VMEM((LOCAL, rows, 2 * HEAD), jnp.bfloat16),
            pltpu.VMEM((d // WIDE, rows, WIDE), jnp.float32),
            dma((3,)),
            dma((2,)),
            dma((LOCAL, 4)),
            dma((LOCAL, 4)),
            dma((LOCAL, 2)),
            dma((LOCAL, 2)),
            dma((LOCAL, 2)),
            dma((1,)),
        ],
        compiler_params=pltpu.CompilerParams(collective_id=0, has_side_effects=True, vmem_limit_bytes=VMEM),
        cost_estimate=pl.CostEstimate(flops=2 * t * d * 3 * HEAD * LOCAL, transcendentals=0, bytes_accessed=2 * (t * d + 3 * d * HEAD * LOCAL)),
        name="attention_half",
    )(x, gain, near, far, wq, wk, wv, wo)


def tables(rows, blocks):
    rate = THETA ** (-np.arange(HALF) / HALF)
    of = lambda places: np.stack([f(places[:, None] * rate) for f in (np.cos, np.sin)]).astype(np.float32)
    return of(np.arange(rows)), of(np.arange(blocks) * rows)


def solution(mesh):
    def step(x, gain, wq, wk, wv, wo):
        near, far = tables(x.shape[0], mesh.shape["sp"])
        return attention_half(x, gain, jnp.asarray(near), jnp.asarray(far), wq, wk, wv, wo)

    tokens, whole = P(("dp", "sp"), None), P(None, None)
    return jax.shard_map(
        step,
        mesh=mesh,
        in_specs=(tokens, P(None), whole, whole, whole, whole),
        out_specs=tokens,
        check_vma=False,
    )
```

```python
import functools

import jax
import jax.numpy as jnp
import numpy as np
from jax import lax
from jax.experimental import pallas as pl
from jax.experimental.pallas import tpu as pltpu
from jax.sharding import PartitionSpec as P

HEAD = 256
HALF = HEAD // 2
THETA = 10000
NEG = -1e30
HIDDEN = 2 * NEG
LOG2E = 1.4426950408889634
SCALE = HEAD**-0.5
E2 = SCALE * LOG2E
VMEM = 67_000_000 // 1024 * 1024
BK = 512
STRIP = 512

def _dot(a, b, ca, cb):
    return lax.dot_general(a, b, (((ca,), (cb,)), ((), ())), preferred_element_type=jnp.float32)


LOCAL = 8
PAIRS = LOCAL // 2
WIDE = 2 * HEAD


def _block(k, v, strips, top_s, mix_s, masks=None):
    values = jnp.concatenate([v.T, jnp.ones((8, k.shape[0]), k.dtype)], axis=0)
    scores = [_dot(k, q, 1, 1) for _, q in strips]
    weights, keeps = [], []
    for n, ((i, _), s) in enumerate(zip(strips, scores)):
        if masks is not None:
            s = jnp.where(masks[n], s, HIDDEN)
        old = top_s[i]
        top = jnp.maximum(old, s.max(axis=0, keepdims=True))
        top_s[i] = top
        weights.append(jnp.exp2((s - top) * E2).astype(k.dtype))
        keeps.append(jnp.exp2((old - top) * E2))
    for (i, _), p, keep in zip(strips, weights, keeps):
        mix_s[i] = mix_s[i] * keep + _dot(values, p, 1, 0)


def _clear(i, top_s, mix_s):
    top_s[i] = jnp.full((1, STRIP), NEG, jnp.float32)
    mix_s[i] = jnp.zeros((HEAD + 8, STRIP), jnp.float32)


def _result(i, top_s, mix_s):
    total = mix_s[i, HEAD : HEAD + 1, :]
    return (mix_s[i, :HEAD, :] * (1 / total)).T.astype(jnp.bfloat16), top_s[i] * SCALE + jnp.log(total)


def _part(i):
    return slice(i * STRIP, (i + 1) * STRIP)


def _main(
    x_ref, gain_ref, near_ref, far_ref, wq_ref, wk_ref, wv_ref, wo_ref, y_ref,
    a_s, w_s, qkv, recv, lse_s, lse_r, top_s, mix_s, cos_ref, sin_ref, o_s, y_s,
    sem_a, sem_w, send_s, recv_s, lsend_s, lrecv_s, out_s, sem_y,
):
    s = lax.axis_index("sp")
    z, c = s // 2, s % 2
    other = s + 1 - 2 * c
    rows = x_ref.shape[0]
    remote = functools.partial(pltpu.make_async_remote_copy, device_id_type=pl.DeviceIdType.MESH)

    def queries_one_down(h):
        return remote(qkv.at[h, 0], recv.at[h, 0], send_s.at[h, 2], recv_s.at[h, 0], device_id={"sp": s - 2})

    def queries_on(h):
        return remote(recv.at[h, 0], recv.at[h, 1], send_s.at[h, 3], recv_s.at[h, 1], device_id={"sp": s - 2})

    def keys_up(h):
        return remote(qkv.at[h, 1], recv.at[h, 2], send_s.at[h, 2], recv_s.at[h, 2], device_id={"sp": s + 2})

    def values_up(h):
        return remote(qkv.at[h, 2], recv.at[h, 3], send_s.at[h, 3], recv_s.at[h, 3], device_id={"sp": s + 2})

    def part_one_up(h):
        return (
            remote(recv.at[h, lax.rem(z + 1, 2)], recv.at[h, 2], send_s.at[h, 0], recv_s.at[h, 2], device_id={"sp": s + 2}),
            remote(lse_s.at[h, 0], lse_r.at[h, 0], lsend_s.at[h, 0], lrecv_s.at[h, 0], device_id={"sp": s + 2}),
        )

    def part_two_up(h):
        return (
            remote(recv.at[h, 1], recv.at[h, 3], send_s.at[h, 1], recv_s.at[h, 3], device_id={"sp": s + 4}),
            remote(lse_s.at[h, 1], lse_r.at[h, 1], lsend_s.at[h, 1], lrecv_s.at[h, 1], device_id={"sp": s + 4}),
        )

    def give(h):
        return remote(qkv.at[h, 0, pl.ds(rows, rows)], o_s.at[h, :, pl.ds(HEAD, HEAD)], out_s.at[h, 0], out_s.at[h, 1], device_id={"sp": other})

    a_in = pltpu.make_async_copy(x_ref, a_s.at[pl.ds(0, rows)], sem_a.at[0])
    a_over = [
        remote(x_ref.at[pl.ds(at, rows // 2)], a_s.at[pl.ds(rows + at, rows // 2)], sem_a.at[1 + n], sem_a.at[3 + n], device_id={"sp": other})
        for n, at in enumerate((0, rows // 2))
    ]

    lower = z < 2
    kind_0 = jnp.where(lower, 1 - c, c)
    kind_1 = jnp.where(lower, 2 - c, 1 - c)
    kind_2 = 3 - kind_0 - kind_1

    def kind_at(j):
        return jnp.where(j == 0, kind_0, jnp.where(j == 1, kind_1, kind_2))

    def start_weights(tile):
        p, j = tile // 3, lax.rem(tile, 3)
        at = pl.ds(pl.multiple_of((c * PAIRS + p) * WIDE, WIDE), WIDE)
        slot, kind = lax.rem(tile, 2), kind_at(j)
        for n, w in enumerate((wq_ref, wk_ref, wv_ref)):

            @pl.when(kind == n)
            def _():
                pltpu.make_async_copy(w.at[:, at], w_s.at[slot], sem_w.at[slot]).start()

    def wait_weights(slot):
        pltpu.make_async_copy(wq_ref.at[:, pl.ds(0, WIDE)], w_s.at[slot], sem_w.at[slot]).wait()

    a_in.start()
    start_weights(jnp.int32(0))
    start_weights(jnp.int32(1))

    barrier = pltpu.get_barrier_semaphore()
    for n in range(1, 8):
        pl.semaphore_signal(barrier, inc=1, device_id={"sp": lax.rem(s + n, 8)}, device_id_type=pl.DeviceIdType.MESH)
    pl.semaphore_wait(barrier, 7)
    for copy in a_over:
        copy.start()

    y_s[...] = jnp.zeros_like(y_s)
    for i, place in enumerate((s, other)):
        cos, sin = far_ref[0, pl.ds(place, 1), :], far_ref[1, pl.ds(place, 1), :]
        here = pl.ds(i * rows, rows)
        cos_ref[here, :] = near_ref[0] * cos - near_ref[1] * sin
        sin_ref[here, :] = near_ref[1] * cos + near_ref[0] * sin

    gain = gain_ref[...].astype(jnp.float32)[None, :]

    def norm(first, count):
        def body(i, _):
            here = pl.ds(pl.multiple_of(first + i * 32, 32), 32)
            wide = a_s[here, :].astype(jnp.float32)
            scale = lax.rsqrt(jnp.mean(wide * wide, -1, keepdims=True) + 1e-6)
            a_s[here, :] = (wide * scale * gain).astype(jnp.bfloat16)

        lax.fori_loop(0, count // 32, body, None, unroll=2)

    a_in.wait()
    norm(0, rows)

    def pass_on(h):
        queries_one_down(h).wait_recv()
        queries_on(h).start()

    def project(p):
        def one_kind(j, _):
            tile = 3 * p + j
            kind = kind_at(j)
            slot = lax.rem(tile, 2)
            wait_weights(slot)

            def half(m, _):
                @pl.when((tile == 0) & (m == 1))
                def _():
                    for n, copy in enumerate(a_over):
                        copy.wait_recv()
                        norm(rows + n * rows // 2, rows // 2)

                here = pl.ds(pl.multiple_of(m * rows, rows), rows)
                t = _dot(a_s[here, :], w_s[slot], 1, 0)
                cos, sin = cos_ref[here, :], sin_ref[here, :]
                for i in range(2):
                    u = t[:, i * HEAD : (i + 1) * HEAD].astype(jnp.bfloat16)

                    @pl.when(kind == 2)
                    def _():
                        qkv[2 * p + i, 2, here, :] = u

                    @pl.when(kind < 2)
                    def _():
                        v = u.astype(jnp.float32)
                        a, b = v[:, :HALF], v[:, HALF:]
                        qkv[2 * p + i, kind, here, :] = jnp.concatenate([a * cos - b * sin, b * cos + a * sin], axis=1).astype(jnp.bfloat16)

            lax.fori_loop(0, 2, half, None)

            @pl.when(tile + 2 < 3 * PAIRS)
            def _():
                start_weights(tile + 2)

            @pl.when((kind == 0) & ((z == 3) | ((z == 2) & (p == 0))))
            def _():
                queries_one_down(2 * p).start()

            @pl.when((z == 2) & (tile == c + 1))
            def _():
                pass_on(0)

            @pl.when((z == 3) & (j == 2))
            def _():
                queries_one_down(2 * p + 1).start()

            @pl.when((z == 0) & (kind == 1))
            def _():
                keys_up(2 * p).start()

            @pl.when((z == 0) & (kind == 2))
            def _():
                values_up(2 * p).start()
                keys_up(2 * p + 1).start()
                values_up(2 * p + 1).start()

        lax.fori_loop(0, 3, one_kind, None)

    def over(ref, h, at, strips):
        for first in range(0, 2 * rows, BK):
            here = slice(first, first + BK)
            _block(ref[h, at, here, :], ref[h, at + 1, here, :], strips(), top_s, mix_s)

    def serve(h):
        def one(n, _):
            @pl.when((z == 1) & (n == 0))
            def _():
                queries_one_down(h).wait_recv()

            @pl.when((z == 1) & (n == 1))
            def _():
                queries_on(h).wait_recv()

            strips = lambda: [(i, recv[h, n, _part(i), :]) for i in range(2)]
            for i in range(2):
                _clear(i, top_s, mix_s)
            over(qkv, h, 1, strips)

            @pl.when(z == 1)
            def _():
                @pl.when(n == 0)
                def _():
                    keys_up(h).wait_recv()
                    values_up(h).wait_recv()

                over(recv, h, 2, strips)

            for i in range(2):
                recv[h, jnp.maximum(n, z - 1), _part(i), :], lse_s[h, n, :, _part(i)] = _result(i, top_s, mix_s)

            @pl.when(n == 0)
            def _():
                for copy in part_one_up(h):
                    copy.start()

            @pl.when(n == 1)
            def _():
                for copy in part_two_up(h):
                    copy.start()

        lax.fori_loop(0, jnp.where(z == 1, 2, 1), one, None)

    def attend_own(h, _):
        one = lambda i: [(i, qkv[h, 0, _part(i), :])]

        @pl.when(z < 2)
        def _():
            for i in range(2):
                _clear(i, top_s, mix_s)

        @pl.when(z == 1)
        def _():
            over(recv, h, 2, lambda: one(0) + one(1))

        @pl.when(z >= 2)
        def _():
            for copy in part_one_up(h):
                copy.wait_recv()
            queries_one_down(h).wait_send()

            @pl.when(z == 2)
            def _():
                for i in range(2):
                    la = lse_r[h, 0, :, _part(i)]
                    top_s[i] = la * (1 / SCALE)
                    mix_s[i, :HEAD, :] = recv[h, 2, _part(i), :].astype(jnp.float32).T
                    mix_s[i, HEAD:, :] = jnp.ones((8, STRIP), jnp.float32)

            @pl.when(z == 3)
            def _():
                for copy in part_two_up(h):
                    copy.wait_recv()
                for i in range(2):
                    la, lb = lse_r[h, 0, :, _part(i)], lse_r[h, 1, :, _part(i)]
                    top = jnp.maximum(la, lb)
                    wa, wb = jnp.exp(la - top), jnp.exp(lb - top)
                    top_s[i] = top * (1 / SCALE)
                    mix_s[i, :HEAD, :] = recv[h, 2, _part(i), :].astype(jnp.float32).T * wa + recv[h, 3, _part(i), :].astype(jnp.float32).T * wb
                    mix_s[i, HEAD:, :] = jnp.broadcast_to(wa + wb, (8, STRIP))

        early = pl.ds(pl.multiple_of(c * STRIP, STRIP), STRIP)
        late = 1 - c
        at = pl.ds(pl.multiple_of(late * STRIP, STRIP), STRIP)
        _block(qkv[h, 1, early, :], qkv[h, 2, early, :], [(late, qkv[h, 0, at, :])], top_s, mix_s)
        seen = lax.broadcasted_iota(jnp.int32, (STRIP, STRIP), 1) >= lax.broadcasted_iota(jnp.int32, (STRIP, STRIP), 0)
        for i in range(2):
            _block(qkv[h, 1, _part(i), :], qkv[h, 2, _part(i), :], one(i), top_s, mix_s, [seen])
        o_s[h, :, :HEAD], _ = _result(0, top_s, mix_s)
        qkv[h, 0, _part(1), :], _ = _result(1, top_s, mix_s)
        give(h).start()

    blocks = wo_ref.shape[1] // WIDE
    x_in = pltpu.make_async_copy(x_ref, a_s.at[pl.ds(0, rows)], sem_a.at[0])

    def start_out(h):
        def body(n, _):
            at = pl.ds(pl.multiple_of(n * WIDE, WIDE), WIDE)
            for side, core in enumerate((c, 1 - c)):
                pltpu.make_async_copy(
                    wo_ref.at[pl.ds(pl.multiple_of((core * LOCAL + h) * HEAD, HEAD), HEAD), at],
                    w_s.at[lax.rem(h, 2), pl.ds(pl.multiple_of(n * WIDE + side * HEAD, HEAD), HEAD)],
                    sem_w.at[lax.rem(h, 2)],
                ).start()

        lax.fori_loop(0, blocks, body, None)

    def out_part(h, _, final):
        slot = lax.rem(h, 2)
        give(h).wait_recv()
        wait_weights(slot)

        if final:
            x_in.wait()

        def body(n, _):
            at = pl.ds(pl.multiple_of(n * WIDE, WIDE), WIDE)
            y_s[n] = y_s[n] + _dot(o_s[h], w_s[slot, at, :], 1, 0)

        def last(n, _):
            at = pl.ds(pl.multiple_of(n * WIDE, WIDE), WIDE)
            y = y_s[n] + _dot(o_s[h], w_s[slot, at, :], 1, 0)
            a_s[pl.ds(rows, rows), at] = (a_s[pl.ds(0, rows), at].astype(jnp.float32) + y).astype(jnp.bfloat16)
            pltpu.make_async_copy(a_s.at[pl.ds(rows, rows), at], y_ref.at[:, at], sem_y.at[0]).start()

        lax.fori_loop(0, blocks, last if final else body, None, unroll=2)

        @pl.when(h < LOCAL - 2)
        def _():
            start_out(h + 2)

    def turn(i, _):
        t = i - 1
        p = t + jnp.where((z == 1) & (c == 1), 1, 0)

        @pl.when((p >= 0) & (p < PAIRS))
        def _():
            project(p)

        @pl.when(p == PAIRS - 1)
        def _():
            x_in.start()
            start_out(jnp.int32(0))
            start_out(jnp.int32(1))

        @pl.when((t >= 0) & (t < LOCAL) & ((z == 1) | (z == 2)))
        def _():
            serve(t)

        @pl.when((z == 2) & (t >= 0) & (t < LOCAL - 1))
        def _():
            queries_one_down(t + 1).start()
            pass_on(t + 1)

        def parts(t):
            return jnp.clip(jnp.where(z == 0, 2 * t - 7, jnp.where(z == 1, jnp.minimum(3 * t - 10, t), t - 2)), 0, LOCAL - 1)

        def heads(t):
            return jnp.clip(jnp.where(z == 0, t + 1, jnp.where(z == 1, jnp.where(t < 3, 0, jnp.minimum(2 * t - 3, t + 1)), t - 1)), 0, LOCAL)

        lax.fori_loop(parts(t - 1), parts(t), functools.partial(out_part, final=False), None)
        lax.fori_loop(heads(t - 1), heads(t), attend_own, None)

    lax.fori_loop(0, LOCAL + 3, turn, None)
    out_part(jnp.int32(LOCAL - 1), None, final=True)
    for copy in a_over:
        copy.wait_send()
    pltpu.make_async_copy(a_s.at[pl.ds(rows, rows)], y_ref, sem_y.at[0]).wait()

    def finish(h, _):
        give(h).wait_send()

        @pl.when(z == 0)
        def _():
            keys_up(h).wait_send()
            values_up(h).wait_send()

        @pl.when((z == 1) | (z == 2))
        def _():
            for copy in part_one_up(h):
                copy.wait_send()

        @pl.when(z == 1)
        def _():
            for copy in part_two_up(h):
                copy.wait_send()

        @pl.when(z == 2)
        def _():
            queries_on(h).wait_send()

    lax.fori_loop(0, LOCAL, finish, None)


def attention_half(x, gain, near, far, wq, wk, wv, wo):
    rows, d = x.shape
    hbm, vmem = pl.BlockSpec(memory_space=pl.ANY), pl.BlockSpec(memory_space=pltpu.VMEM)
    dma = pltpu.SemaphoreType.DMA
    t = 2 * rows
    return pl.pallas_call(
        _main,
        in_specs=[hbm, vmem, vmem, vmem, hbm, hbm, hbm, hbm],
        out_specs=hbm,
        out_shape=jax.ShapeDtypeStruct((rows, d), jnp.bfloat16),
        scratch_shapes=[
            pltpu.VMEM((t, d), jnp.bfloat16),
            pltpu.VMEM((2, d, WIDE), jnp.bfloat16),
            pltpu.VMEM((LOCAL, 3, t, HEAD), jnp.bfloat16),
            pltpu.VMEM((LOCAL, 4, t, HEAD), jnp.bfloat16),
            pltpu.VMEM((LOCAL, 2, 1, t), jnp.float32),
            pltpu.VMEM((LOCAL, 2, 1, t), jnp.float32),
            pltpu.VMEM((2, 1, STRIP), jnp.float32),
            pltpu.VMEM((2, HEAD + 8, STRIP), jnp.float32),
            pltpu.VMEM((t, HALF), jnp.float32),
            pltpu.VMEM((t, HALF), jnp.float32),
            pltpu.VMEM((LOCAL, rows, 2 * HEAD), jnp.bfloat16),
            pltpu.VMEM((d // WIDE, rows, WIDE), jnp.float32),
            dma((5,)),
            dma((2,)),
            dma((LOCAL, 4)),
            dma((LOCAL, 4)),
            dma((LOCAL, 2)),
            dma((LOCAL, 2)),
            dma((LOCAL, 2)),
            dma((1,)),
        ],
        compiler_params=pltpu.CompilerParams(collective_id=0, has_side_effects=True, vmem_limit_bytes=VMEM),
        cost_estimate=pl.CostEstimate(flops=2 * t * d * 3 * HEAD * LOCAL, transcendentals=0, bytes_accessed=2 * (t * d + 3 * d * HEAD * LOCAL)),
        name="attention_half",
    )(x, gain, near, far, wq, wk, wv, wo)


def tables(rows, blocks):
    rate = THETA ** (-np.arange(HALF) / HALF)
    of = lambda places: np.stack([f(places[:, None] * rate) for f in (np.cos, np.sin)]).astype(np.float32)
    return of(np.arange(rows)), of(np.arange(blocks) * rows)


def solution(mesh):
    def step(x, gain, wq, wk, wv, wo):
        near, far = tables(x.shape[0], mesh.shape["sp"])
        return attention_half(x, gain, jnp.asarray(near), jnp.asarray(far), wq, wk, wv, wo)

    tokens, whole = P(("dp", "sp"), None), P(None, None)
    return jax.shard_map(
        step,
        mesh=mesh,
        in_specs=(tokens, P(None), whole, whole, whole, whole),
        out_specs=tokens,
        check_vma=False,
    )
```

```python
import functools

import jax
import jax.numpy as jnp
import numpy as np
from jax import lax
from jax.experimental import pallas as pl
from jax.experimental.pallas import tpu as pltpu
from jax.sharding import PartitionSpec as P

HEAD = 256
HALF = HEAD // 2
THETA = 10000
NEG = -1e30
HIDDEN = 2 * NEG
LOG2E = 1.4426950408889634
SCALE = HEAD**-0.5
E2 = SCALE * LOG2E
VMEM = 67_000_000 // 1024 * 1024
BK = 512
STRIP = 512

def _dot(a, b, ca, cb):
    return lax.dot_general(a, b, (((ca,), (cb,)), ((), ())), preferred_element_type=jnp.float32)


LOCAL = 8
PAIRS = LOCAL // 2
WIDE = 2 * HEAD


def _block(k, v, strips, top_s, mix_s, masks=None):
    values = jnp.concatenate([v.T, jnp.ones((8, k.shape[0]), k.dtype)], axis=0)
    scores = [_dot(k, q, 1, 1) for _, q in strips]
    weights, keeps = [], []
    for n, ((i, _), s) in enumerate(zip(strips, scores)):
        if masks is not None:
            s = jnp.where(masks[n], s, HIDDEN)
        old = top_s[i]
        top = jnp.maximum(old, s.max(axis=0, keepdims=True))
        top_s[i] = top
        weights.append(jnp.exp2((s - top) * E2).astype(k.dtype))
        keeps.append(jnp.exp2((old - top) * E2))
    for (i, _), p, keep in zip(strips, weights, keeps):
        mix_s[i] = mix_s[i] * keep + _dot(values, p, 1, 0)


def _clear(i, top_s, mix_s):
    top_s[i] = jnp.full((1, STRIP), NEG, jnp.float32)
    mix_s[i] = jnp.zeros((HEAD + 8, STRIP), jnp.float32)


def _result(i, top_s, mix_s):
    total = mix_s[i, HEAD : HEAD + 1, :]
    return (mix_s[i, :HEAD, :] * (1 / total)).T.astype(jnp.bfloat16), top_s[i] * SCALE + jnp.log(total)


def _part(i):
    return slice(i * STRIP, (i + 1) * STRIP)


def _main(
    x_ref, gain_ref, near_ref, far_ref, wq_ref, wk_ref, wv_ref, wo_ref, y_ref,
    a_s, w_s, qkv, recv, lse_s, lse_r, top_s, mix_s, cos_ref, sin_ref, o_s, y_s,
    sem_a, sem_w, send_s, recv_s, lsend_s, lrecv_s, out_s, sem_y,
):
    s = lax.axis_index("sp")
    z, c = s // 2, s % 2
    other = s + 1 - 2 * c
    rows = x_ref.shape[0]
    remote = functools.partial(pltpu.make_async_remote_copy, device_id_type=pl.DeviceIdType.MESH)

    def queries_one_down(h):
        return remote(qkv.at[h, 0], recv.at[h, 0], send_s.at[h, 2], recv_s.at[h, 0], device_id={"sp": s - 2})

    def queries_on(h):
        return remote(recv.at[h, 0], recv.at[h, 1], send_s.at[h, 3], recv_s.at[h, 1], device_id={"sp": s - 2})

    def keys_up(h):
        return remote(qkv.at[h, 1], recv.at[h, 2], send_s.at[h, 2], recv_s.at[h, 2], device_id={"sp": s + 2})

    def values_up(h):
        return remote(qkv.at[h, 2], recv.at[h, 3], send_s.at[h, 3], recv_s.at[h, 3], device_id={"sp": s + 2})

    def part_one_up(h):
        return (
            remote(recv.at[h, lax.rem(z + 1, 2)], recv.at[h, 2], send_s.at[h, 0], recv_s.at[h, 2], device_id={"sp": s + 2}),
            remote(lse_s.at[h, 0], lse_r.at[h, 0], lsend_s.at[h, 0], lrecv_s.at[h, 0], device_id={"sp": s + 2}),
        )

    def part_two_up(h):
        return (
            remote(recv.at[h, 1], recv.at[h, 3], send_s.at[h, 1], recv_s.at[h, 3], device_id={"sp": s + 4}),
            remote(lse_s.at[h, 1], lse_r.at[h, 1], lsend_s.at[h, 1], lrecv_s.at[h, 1], device_id={"sp": s + 4}),
        )

    def give(h):
        return remote(qkv.at[h, 0, pl.ds(rows, rows)], o_s.at[h, :, pl.ds(HEAD, HEAD)], out_s.at[h, 0], out_s.at[h, 1], device_id={"sp": other})

    a_in = pltpu.make_async_copy(x_ref, a_s.at[pl.ds(0, rows)], sem_a.at[0])
    a_over = [
        remote(x_ref.at[pl.ds(at, rows // 2)], a_s.at[pl.ds(rows + at, rows // 2)], sem_a.at[1 + n], sem_a.at[3 + n], device_id={"sp": other})
        for n, at in enumerate((0, rows // 2))
    ]

    lower = z < 2
    kind_0 = jnp.where(lower, 1 - c, c)
    kind_1 = jnp.where(lower, 2 - c, 1 - c)
    kind_2 = 3 - kind_0 - kind_1

    def kind_at(j):
        return jnp.where(j == 0, kind_0, jnp.where(j == 1, kind_1, kind_2))

    def start_weights(tile):
        p, j = tile // 3, lax.rem(tile, 3)
        at = pl.ds(pl.multiple_of((c * PAIRS + p) * WIDE, WIDE), WIDE)
        slot, kind = lax.rem(tile, 2), kind_at(j)
        for n, w in enumerate((wq_ref, wk_ref, wv_ref)):

            @pl.when(kind == n)
            def _():
                pltpu.make_async_copy(w.at[:, at], w_s.at[slot], sem_w.at[slot]).start()

    def wait_weights(slot):
        pltpu.make_async_copy(wq_ref.at[:, pl.ds(0, WIDE)], w_s.at[slot], sem_w.at[slot]).wait()

    a_in.start()
    start_weights(jnp.int32(0))
    start_weights(jnp.int32(1))

    barrier = pltpu.get_barrier_semaphore()
    for n in range(1, 8):
        pl.semaphore_signal(barrier, inc=1, device_id={"sp": lax.rem(s + n, 8)}, device_id_type=pl.DeviceIdType.MESH)
    pl.semaphore_wait(barrier, 7)
    for copy in a_over:
        copy.start()

    y_s[...] = jnp.zeros_like(y_s)
    for i, place in enumerate((s, other)):
        cos, sin = far_ref[0, pl.ds(place, 1), :], far_ref[1, pl.ds(place, 1), :]
        here = pl.ds(i * rows, rows)
        cos_ref[here, :] = near_ref[0] * cos - near_ref[1] * sin
        sin_ref[here, :] = near_ref[1] * cos + near_ref[0] * sin

    gain = gain_ref[...].astype(jnp.float32)[None, :]

    def norm(first, count):
        def body(i, _):
            here = pl.ds(pl.multiple_of(first + i * 32, 32), 32)
            wide = a_s[here, :].astype(jnp.float32)
            scale = lax.rsqrt(jnp.mean(wide * wide, -1, keepdims=True) + 1e-6)
            a_s[here, :] = (wide * scale * gain).astype(jnp.bfloat16)

        lax.fori_loop(0, count // 32, body, None, unroll=2)

    a_in.wait()
    norm(0, rows)

    def pass_on(h):
        queries_one_down(h).wait_recv()
        queries_on(h).start()

    def project(p):
        def one_kind(j, _):
            tile = 3 * p + j
            kind = kind_at(j)
            slot = lax.rem(tile, 2)
            wait_weights(slot)

            def half(m, _):
                @pl.when((tile == 0) & (m == 1))
                def _():
                    for n, copy in enumerate(a_over):
                        copy.wait_recv()
                        norm(rows + n * rows // 2, rows // 2)

                here = pl.ds(pl.multiple_of(m * rows, rows), rows)
                t = _dot(a_s[here, :], w_s[slot], 1, 0)
                cos, sin = cos_ref[here, :], sin_ref[here, :]
                for i in range(2):
                    u = t[:, i * HEAD : (i + 1) * HEAD].astype(jnp.bfloat16)

                    @pl.when(kind == 2)
                    def _():
                        qkv[2 * p + i, 2, here, :] = u

                    @pl.when(kind < 2)
                    def _():
                        v = u.astype(jnp.float32)
                        a, b = v[:, :HALF], v[:, HALF:]
                        qkv[2 * p + i, kind, here, :] = jnp.concatenate([a * cos - b * sin, b * cos + a * sin], axis=1).astype(jnp.bfloat16)

            lax.fori_loop(0, 2, half, None)

            @pl.when(tile + 2 < 3 * PAIRS)
            def _():
                start_weights(tile + 2)

            @pl.when((kind == 0) & ((z == 3) | ((z == 2) & (p == 0))))
            def _():
                queries_one_down(2 * p).start()

            @pl.when((z == 2) & (tile == c + 1))
            def _():
                pass_on(0)

            @pl.when((z == 3) & (j == 2))
            def _():
                queries_one_down(2 * p + 1).start()

            @pl.when((z == 0) & (kind == 1))
            def _():
                keys_up(2 * p).start()

            @pl.when((z == 0) & (kind == 2))
            def _():
                values_up(2 * p).start()
                keys_up(2 * p + 1).start()
                values_up(2 * p + 1).start()

        lax.fori_loop(0, 3, one_kind, None)

    def over(ref, h, at, strips):
        for first in range(0, 2 * rows, BK):
            here = slice(first, first + BK)
            _block(ref[h, at, here, :], ref[h, at + 1, here, :], strips(), top_s, mix_s)

    def serve(h):
        def one(n, _):
            @pl.when((z == 1) & (n == 0))
            def _():
                queries_one_down(h).wait_recv()

            @pl.when((z == 1) & (n == 1))
            def _():
                queries_on(h).wait_recv()

            strips = lambda: [(i, recv[h, n, _part(i), :]) for i in range(2)]
            for i in range(2):
                _clear(i, top_s, mix_s)
            over(qkv, h, 1, strips)

            @pl.when(z == 1)
            def _():
                @pl.when(n == 0)
                def _():
                    keys_up(h).wait_recv()
                    values_up(h).wait_recv()

                over(recv, h, 2, strips)

            for i in range(2):
                recv[h, jnp.maximum(n, z - 1), _part(i), :], lse_s[h, n, :, _part(i)] = _result(i, top_s, mix_s)

            @pl.when(n == 0)
            def _():
                for copy in part_one_up(h):
                    copy.start()

            @pl.when(n == 1)
            def _():
                for copy in part_two_up(h):
                    copy.start()

        lax.fori_loop(0, jnp.where(z == 1, 2, 1), one, None)

    def attend_own(h, _):
        one = lambda i: [(i, qkv[h, 0, _part(i), :])]

        @pl.when(z < 2)
        def _():
            for i in range(2):
                _clear(i, top_s, mix_s)

        @pl.when(z == 1)
        def _():
            over(recv, h, 2, lambda: one(0) + one(1))

        @pl.when(z >= 2)
        def _():
            for copy in part_one_up(h):
                copy.wait_recv()
            queries_one_down(h).wait_send()

            @pl.when(z == 2)
            def _():
                for i in range(2):
                    la = lse_r[h, 0, :, _part(i)]
                    top_s[i] = la * (1 / SCALE)
                    mix_s[i, :HEAD, :] = recv[h, 2, _part(i), :].astype(jnp.float32).T
                    mix_s[i, HEAD:, :] = jnp.ones((8, STRIP), jnp.float32)

            @pl.when(z == 3)
            def _():
                for copy in part_two_up(h):
                    copy.wait_recv()
                for i in range(2):
                    la, lb = lse_r[h, 0, :, _part(i)], lse_r[h, 1, :, _part(i)]
                    top = jnp.maximum(la, lb)
                    wa, wb = jnp.exp(la - top), jnp.exp(lb - top)
                    top_s[i] = top * (1 / SCALE)
                    mix_s[i, :HEAD, :] = recv[h, 2, _part(i), :].astype(jnp.float32).T * wa + recv[h, 3, _part(i), :].astype(jnp.float32).T * wb
                    mix_s[i, HEAD:, :] = jnp.broadcast_to(wa + wb, (8, STRIP))

        early = pl.ds(pl.multiple_of(c * STRIP, STRIP), STRIP)
        late = 1 - c
        at = pl.ds(pl.multiple_of(late * STRIP, STRIP), STRIP)
        _block(qkv[h, 1, early, :], qkv[h, 2, early, :], [(late, qkv[h, 0, at, :])], top_s, mix_s)
        seen = lax.broadcasted_iota(jnp.int32, (STRIP, STRIP), 1) >= lax.broadcasted_iota(jnp.int32, (STRIP, STRIP), 0)
        for i in range(2):
            _block(qkv[h, 1, _part(i), :], qkv[h, 2, _part(i), :], one(i), top_s, mix_s, [seen])
        o_s[h, :, :HEAD], _ = _result(0, top_s, mix_s)
        qkv[h, 0, _part(1), :], _ = _result(1, top_s, mix_s)
        give(h).start()

    blocks = wo_ref.shape[1] // WIDE
    x_in = pltpu.make_async_copy(x_ref, a_s.at[pl.ds(0, rows)], sem_a.at[0])

    def start_out(h):
        def body(n, _):
            at = pl.ds(pl.multiple_of(n * WIDE, WIDE), WIDE)
            for side, core in enumerate((c, 1 - c)):
                pltpu.make_async_copy(
                    wo_ref.at[pl.ds(pl.multiple_of((core * LOCAL + h) * HEAD, HEAD), HEAD), at],
                    w_s.at[lax.rem(h, 2), pl.ds(pl.multiple_of(n * WIDE + side * HEAD, HEAD), HEAD)],
                    sem_w.at[lax.rem(h, 2)],
                ).start()

        lax.fori_loop(0, blocks, body, None)

    def out_part(h, _, final):
        slot = lax.rem(h, 2)
        give(h).wait_recv()
        wait_weights(slot)

        if final:
            x_in.wait()

        def body(n, _):
            at = pl.ds(pl.multiple_of(n * WIDE, WIDE), WIDE)
            y_s[n] = y_s[n] + _dot(o_s[h], w_s[slot, at, :], 1, 0)

        def last(n, _):
            at = pl.ds(pl.multiple_of(n * WIDE, WIDE), WIDE)
            y = y_s[n] + _dot(o_s[h], w_s[slot, at, :], 1, 0)
            a_s[pl.ds(rows, rows), at] = (a_s[pl.ds(0, rows), at].astype(jnp.float32) + y).astype(jnp.bfloat16)
            pltpu.make_async_copy(a_s.at[pl.ds(rows, rows), at], y_ref.at[:, at], sem_y.at[0]).start()

        lax.fori_loop(0, blocks, last if final else body, None, unroll=2)

        @pl.when(h < LOCAL - 2)
        def _():
            start_out(h + 2)

    def turn(i, _):
        t = i - 1
        u = t + jnp.where(z == 1, c, 0)
        spread = (z == 1) & (c == 0) & (u >= 2)
        p = jnp.where(spread, (u + 1) // 2, u)

        @pl.when((u >= 0) & (p < PAIRS) & (jnp.logical_not(spread) | (u % 2 == 1)))
        def _():
            project(p)

        @pl.when((p == PAIRS - 1) & (jnp.logical_not(spread) | (u % 2 == 1)))
        def _():
            x_in.start()
            start_out(jnp.int32(0))
            start_out(jnp.int32(1))

        @pl.when((t >= 0) & (t < LOCAL) & ((z == 1) | (z == 2)))
        def _():
            serve(t)

        @pl.when((z == 2) & (t >= 0) & (t < LOCAL - 1))
        def _():
            queries_one_down(t + 1).start()
            pass_on(t + 1)

        def parts(t):
            one = jnp.where(c == 0, 3 * t - 15, jnp.minimum(3 * t - 10, t))
            return jnp.clip(jnp.where(z == 0, 2 * t - 7, jnp.where(z == 1, one, t - 2)), 0, LOCAL - 1)

        def heads(t):
            one = jnp.where(c == 0, jnp.maximum(t + 1, 0) // 2 * 2, jnp.where(t < 3, 0, jnp.minimum(2 * t - 3, t + 1)))
            return jnp.clip(jnp.where(z == 0, t + 1, jnp.where(z == 1, one, t - 1)), 0, LOCAL)

        lax.fori_loop(parts(t - 1), parts(t), functools.partial(out_part, final=False), None)
        lax.fori_loop(heads(t - 1), heads(t), attend_own, None)

    lax.fori_loop(0, LOCAL + 3, turn, None)
    out_part(jnp.int32(LOCAL - 1), None, final=True)
    for copy in a_over:
        copy.wait_send()
    pltpu.make_async_copy(a_s.at[pl.ds(rows, rows)], y_ref, sem_y.at[0]).wait()

    def finish(h, _):
        give(h).wait_send()

        @pl.when(z == 0)
        def _():
            keys_up(h).wait_send()
            values_up(h).wait_send()

        @pl.when((z == 1) | (z == 2))
        def _():
            for copy in part_one_up(h):
                copy.wait_send()

        @pl.when(z == 1)
        def _():
            for copy in part_two_up(h):
                copy.wait_send()

        @pl.when(z == 2)
        def _():
            queries_on(h).wait_send()

    lax.fori_loop(0, LOCAL, finish, None)


def attention_half(x, gain, near, far, wq, wk, wv, wo):
    rows, d = x.shape
    hbm, vmem = pl.BlockSpec(memory_space=pl.ANY), pl.BlockSpec(memory_space=pltpu.VMEM)
    dma = pltpu.SemaphoreType.DMA
    t = 2 * rows
    return pl.pallas_call(
        _main,
        in_specs=[hbm, vmem, vmem, vmem, hbm, hbm, hbm, hbm],
        out_specs=hbm,
        out_shape=jax.ShapeDtypeStruct((rows, d), jnp.bfloat16),
        scratch_shapes=[
            pltpu.VMEM((t, d), jnp.bfloat16),
            pltpu.VMEM((2, d, WIDE), jnp.bfloat16),
            pltpu.VMEM((LOCAL, 3, t, HEAD), jnp.bfloat16),
            pltpu.VMEM((LOCAL, 4, t, HEAD), jnp.bfloat16),
            pltpu.VMEM((LOCAL, 2, 1, t), jnp.float32),
            pltpu.VMEM((LOCAL, 2, 1, t), jnp.float32),
            pltpu.VMEM((2, 1, STRIP), jnp.float32),
            pltpu.VMEM((2, HEAD + 8, STRIP), jnp.float32),
            pltpu.VMEM((t, HALF), jnp.float32),
            pltpu.VMEM((t, HALF), jnp.float32),
            pltpu.VMEM((LOCAL, rows, 2 * HEAD), jnp.bfloat16),
            pltpu.VMEM((d // WIDE, rows, WIDE), jnp.float32),
            dma((5,)),
            dma((2,)),
            dma((LOCAL, 4)),
            dma((LOCAL, 4)),
            dma((LOCAL, 2)),
            dma((LOCAL, 2)),
            dma((LOCAL, 2)),
            dma((1,)),
        ],
        compiler_params=pltpu.CompilerParams(collective_id=0, has_side_effects=True, vmem_limit_bytes=VMEM),
        cost_estimate=pl.CostEstimate(flops=2 * t * d * 3 * HEAD * LOCAL, transcendentals=0, bytes_accessed=2 * (t * d + 3 * d * HEAD * LOCAL)),
        name="attention_half",
    )(x, gain, near, far, wq, wk, wv, wo)


def tables(rows, blocks):
    rate = THETA ** (-np.arange(HALF) / HALF)
    of = lambda places: np.stack([f(places[:, None] * rate) for f in (np.cos, np.sin)]).astype(np.float32)
    return of(np.arange(rows)), of(np.arange(blocks) * rows)


def solution(mesh):
    def step(x, gain, wq, wk, wv, wo):
        near, far = tables(x.shape[0], mesh.shape["sp"])
        return attention_half(x, gain, jnp.asarray(near), jnp.asarray(far), wq, wk, wv, wo)

    tokens, whole = P(("dp", "sp"), None), P(None, None)
    return jax.shard_map(
        step,
        mesh=mesh,
        in_specs=(tokens, P(None), whole, whole, whole, whole),
        out_specs=tokens,
        check_vma=False,
    )
```
